512 devices in a mesh: shot: 64 (over x, y, core), det: 8 (over z).
Axes of the slice: x: 4, y: 8, z: 8, core: 2. Of those that a mesh axis runs over, the one named last changes fastest.
Arguments:
- events: int32 [65536, 8192], P('shot', 'det'), may hold values from 0 to 1, as said below
- pair_patches: int32 [8, 26, 2], P('det'), may hold values from 0 to 7, as said below
- pair_owners: int32 [8, 26, 2], P('det'), may hold values from 0 to 63, as said below
- triples: int32 [8, 256, 3], P('det'), may hold values from 0 to 1023, as said below
Outputs:
- intra_rates: float32 [64, 128, 128], P('det', 'shot')
- boundary_rates: float32 [8, 64, 2, 128, 128], P('det', 'shot')
- detector_load: float32 [64, 128], P(None, 'shot')
- triple_cumulant: float32 [8, 256], P('det')
The draws below stay inside these ranges and needn't reach their ends.
Inputs may be any that keep to these rules, and one draw needn't show every extreme that they name: events[s, i] is 1 where detector i fired in shot s, else 0. `pair_patches`: row d lists 26 blocks of panel d, each naming two different patches of the panel; no two blocks name the same two patches. `pair_owners`: of the 52 owner entries of one panel, no shot index is named more than 2 times, and in every panel some index is named exactly 2 times. `triples`: each triple holds three different detector indices of the panel in increasing order.
All inputs are finite; a program needn't handle non-finite values.
Results may differ from the reference program's by a relative error of at most 0.0003.
Values sent between devices are 32-bit elements; how exact they have to be, the bound alone decides.
No kernel may reach another device: no remote copies, remote signals or barrier semaphores. Data moves between devices by JAX's collectives and lax.ppermute only.
A program may use at most 64 MiB of HBM per device.

```python
import jax
import jax.numpy as jnp
import numpy as np
from jax import lax

SHOT_DEV = 1024
PB = 128
PATCH_DEV = 8
PAIRS = 26
TRIPLES = 256
DET_DEV = 1024
PATCHES = 64
DETS = 8192
SHOTS = 65536
RECV = 2
N_SHOT = 64
N_DET = 8


def draw_events(key, part):
    key_list = jax.random.split(jax.random.fold_in(key, 11), 5)
    exponents = jax.random.randint(key_list[0], (DETS,), 3, 8)
    noisy_mask = jax.random.randint(key_list[1], (DETS,), 0, 32) == 0
    base_level = jnp.right_shift(jnp.int32(1 << 20), exponents)
    edge_level = jnp.right_shift(jnp.int32(1 << 20), jax.random.randint(key_list[2], (DETS,), 5, 10))
    hyper_level = jnp.right_shift(jnp.int32(1 << 20), jax.random.randint(key_list[3], (DETS,), 6, 10))
    span_steps = max(N_SHOT - 1, 1)

    def shot_block(block_index):
        block_keys = jax.random.split(jax.random.fold_in(key_list[4], block_index), 3)
        growth = span_steps + 2 * block_index
        noise_level = jnp.where(noisy_mask, 471859, base_level * growth // span_steps)
        single = jax.random.randint(block_keys[0], (SHOT_DEV, DETS), 0, 1 << 20) < noise_level[None, :]
        pairwise = jax.random.randint(block_keys[1], (SHOT_DEV, DETS), 0, 1 << 20) < (edge_level * growth // span_steps)[None, :]
        higher = jax.random.randint(block_keys[2], (SHOT_DEV, DETS), 0, 1 << 20) < (hyper_level * growth // span_steps)[None, :]
        flipped = single ^ pairwise ^ jnp.roll(pairwise, 1, axis=1) ^ higher ^ jnp.roll(higher, 1, axis=1) ^ jnp.roll(higher, 3, axis=1)
        return flipped.astype(jnp.int32)
    blocks = lax.map(shot_block, jnp.arange(N_SHOT, dtype=jnp.int32))
    return blocks.reshape(N_SHOT * SHOT_DEV, DETS)


def draw_pair_patches(key, part):
    first_np, second_np = np.triu_indices(PATCH_DEV, 1)
    pair_table = jnp.stack([jnp.asarray(first_np, jnp.int32), jnp.asarray(second_np, jnp.int32)], axis=1)

    def one_panel(panel_index):
        panel_key = jax.random.fold_in(jax.random.fold_in(key, 23), panel_index)
        first_key, second_key = jax.random.split(panel_key)
        picked = jax.random.permutation(first_key, pair_table.shape[0])[:PAIRS]
        chosen = pair_table[picked]
        reverse_bit = jax.random.randint(second_key, (PAIRS, 1), 0, 2)
        return jnp.where(reverse_bit == 1, chosen[:, ::-1], chosen).astype(jnp.int32)
    return lax.map(one_panel, jnp.arange(N_DET, dtype=jnp.int32))


def draw_pair_owners(key, part):

    def one_panel(panel_index):
        panel_key = jax.random.fold_in(jax.random.fold_in(key, 37), panel_index)
        first_key, second_key, third_key = jax.random.split(panel_key, 3)
        favored = jax.random.randint(first_key, (), 0, N_SHOT)
        spread = jax.random.permutation(second_key, (N_SHOT - 1) * RECV)[:2 * PAIRS - RECV] // RECV
        spread = spread + (spread >= favored).astype(jnp.int32)
        entries = jnp.concatenate([jnp.full((RECV,), favored, jnp.int32), spread.astype(jnp.int32)])
        entries = jax.random.permutation(third_key, entries)
        return entries.reshape(PAIRS, 2).astype(jnp.int32)
    return lax.map(one_panel, jnp.arange(N_DET, dtype=jnp.int32))


def draw_triples(key, part):
    first_key, second_key, third_key = jax.random.split(jax.random.fold_in(key, 53), 3)
    starts = jax.random.randint(first_key, (N_DET, TRIPLES), 0, PATCH_DEV * PB - 4)
    step_one = jax.random.randint(second_key, (N_DET, TRIPLES), 1, 3)
    step_two = jax.random.randint(third_key, (N_DET, TRIPLES), 1, 3)
    return jnp.stack([starts, starts + step_one, starts + step_one + step_two], axis=-1).astype(jnp.int32)


def setup_inputs(seed: int = 0) -> dict:
    keys = jax.random.split(jax.random.key(seed), 5)
    return {
        "events": draw_events(jax.random.fold_in(keys[4], 71), 0),
        "pair_patches": draw_pair_patches(jax.random.fold_in(keys[4], 71), 0),
        "pair_owners": draw_pair_owners(jax.random.fold_in(keys[4], 71), 0),
        "triples": draw_triples(jax.random.fold_in(keys[4], 71), 0),
    }


def fit_rates(coincide, row_count, col_count, shot_total):
    inverse = 1.0 / shot_total
    joint_rate = coincide * inverse
    row_rate = row_count[..., :, None] * inverse
    col_rate = col_count[..., None, :] * inverse
    denominator = jnp.maximum(1.0 - 2.0 * row_rate - 2.0 * col_rate + 4.0 * joint_rate, 0.25)
    excess = (joint_rate - row_rate * col_rate) / denominator
    return 100.0 * (0.5 - 0.5 * jnp.sqrt(jnp.maximum(1.0 - 4.0 * excess, 0.04)))

def route_table(owner_row, shot_count, recv_slots):
    owner_ids = jnp.arange(shot_count, dtype=jnp.int32)
    hit = owner_row[None, :] == owner_ids[:, None]
    rank = jnp.cumsum(hit.astype(jnp.int32), axis=1) - 1
    slot_ids = jnp.arange(recv_slots, dtype=jnp.int32)
    chosen = hit[:, None, :] & (rank[:, None, :] == slot_ids[None, :, None])
    entry_pair = jnp.arange(owner_row.shape[0], dtype=jnp.int32) // 2
    pair_slot = lax.optimization_barrier(jnp.sum(jnp.where(chosen, entry_pair[None, None, :], 0), axis=2)).astype(jnp.int32)
    valid = jnp.any(chosen, axis=2).astype(jnp.float32)
    return (pair_slot, valid)

def reference(events, pair_patches, pair_owners, triples):
    shot_total = float(SHOTS)
    inverse = 1.0 / shot_total
    counts = lax.optimization_barrier(jnp.sum(events, axis=0)).astype(jnp.float32)
    patch_counts = counts.reshape(PATCHES, PB)

    def patch_gram(patch_index):
        columns = lax.dynamic_slice_in_dim(events, (patch_index * PB).astype(jnp.int32), PB, 1).astype(jnp.float32)
        return jnp.dot(columns.T, columns, precision=lax.Precision.HIGHEST, preferred_element_type=jnp.float32)
    grams = lax.map(patch_gram, jnp.arange(PATCHES, dtype=jnp.int32))
    intra_rates = fit_rates(grams, patch_counts, patch_counts, shot_total)
    detector_load = lax.optimization_barrier(jnp.sum(intra_rates, axis=2))
    offsets = jnp.arange(N_DET, dtype=jnp.int32)[:, None, None] * PATCH_DEV
    pair_ends = (pair_patches + offsets).reshape(N_DET * PAIRS, 2).astype(jnp.int32)

    def pair_gram(ends):
        first_columns = lax.dynamic_slice_in_dim(events, (ends[0] * PB).astype(jnp.int32), PB, 1).astype(jnp.float32)
        second_columns = lax.dynamic_slice_in_dim(events, (ends[1] * PB).astype(jnp.int32), PB, 1).astype(jnp.float32)
        return jnp.dot(first_columns.T, second_columns, precision=lax.Precision.HIGHEST, preferred_element_type=jnp.float32)
    pair_grams = lax.map(pair_gram, pair_ends)
    pair_rates = fit_rates(pair_grams, patch_counts[pair_ends[:, 0]], patch_counts[pair_ends[:, 1]], shot_total)
    pair_slot, valid = jax.vmap(lambda owner_row: route_table(owner_row, N_SHOT, RECV))(pair_owners.reshape(N_DET, 2 * PAIRS))
    flat_index = (jnp.arange(N_DET, dtype=jnp.int32)[:, None, None] * PAIRS + pair_slot).reshape(-1)
    boundary_rates = jnp.take(pair_rates, flat_index, axis=0).reshape(N_DET, N_SHOT, RECV, PB, PB)
    boundary_rates = boundary_rates * valid[:, :, :, None, None]
    global_triples = (triples + jnp.arange(N_DET, dtype=jnp.int32)[:, None, None] * DET_DEV).astype(jnp.int32)

    def triple_sums(index_set):
        picked = jnp.take(events, index_set.reshape(-1), axis=1).astype(jnp.float32).reshape(SHOTS, TRIPLES, 3)
        first_bit = picked[:, :, 0]
        second_bit = picked[:, :, 1]
        third_bit = picked[:, :, 2]
        return jnp.stack([lax.optimization_barrier(jnp.sum(first_bit * second_bit, axis=0)), lax.optimization_barrier(jnp.sum(first_bit * third_bit, axis=0)), lax.optimization_barrier(jnp.sum(second_bit * third_bit, axis=0)), lax.optimization_barrier(jnp.sum(first_bit * second_bit * third_bit, axis=0))])
    moments = lax.map(triple_sums, global_triples) * inverse
    means = counts[global_triples] * inverse
    mean_first = means[:, :, 0]
    mean_second = means[:, :, 1]
    mean_third = means[:, :, 2]
    kappa = moments[:, 3] - moments[:, 0] * mean_third - moments[:, 1] * mean_second - moments[:, 2] * mean_first + 2.0 * mean_first * mean_second * mean_third
    triple_cumulant = 1000.0 * kappa
    return (intra_rates, boundary_rates, detector_load, triple_cumulant)
```

```python
import functools

import jax
import jax.numpy as jnp
from jax import lax
from jax.experimental import pallas as pl
from jax.experimental.pallas import tpu as pltpu
from jax.sharding import Mesh
from jax.sharding import PartitionSpec as P

PB = 128
SHOT = ("shot_0", "shot_1", "shot_2")


def fit(joint, rows, cols, inverse):
    u = joint * inverse
    x = rows * inverse
    y = cols * inverse
    den = jnp.maximum(1.0 - 2.0 * x - 2.0 * y + 4.0 * u, 0.25)
    q = (u - x * y) / den
    return 100.0 * (0.5 - 0.5 * jnp.sqrt(jnp.maximum(1.0 - 4.0 * q, 0.04)))


def iota(shape, dim):
    return lax.broadcasted_iota(jnp.int32, shape, dim)


def ordered(pairs, k):
    return jnp.minimum(pairs[0, k], pairs[1, k]), jnp.maximum(pairs[0, k], pairs[1, k])


def count_kernel(
    core, pairs, triple_rows, events, keep, send,
    raw, bits, flipped, grams, picker, sems,
    *, chunks, patches, pair_count, near, far, rows_own, vector_rows,
):
    shots, dets = raw.shape
    step = shots // chunks
    triple_count = triple_rows.shape[2]
    halves = triple_count // PB
    copies = [
        pltpu.make_async_copy(events.at[pl.ds(i * step, step)], raw.at[pl.ds(i * step, step)], sems.at[i])
        for i in range(chunks)
    ]
    for copy in copies:
        copy.start()
    detector = iota((dets, triple_count), 0)
    for m in range(3):
        hit = detector == triple_rows[m]
        picker[:, m * triple_count : (m + 1) * triple_count] = jnp.where(hit, 1.0, 0.0).astype(jnp.bfloat16)
    counts = jnp.zeros((1, dets), jnp.float32)
    sums = [jnp.zeros((1, triple_count), jnp.float32) for _ in range(7)]
    wide = 2 * PB

    def add_grams(first, last, fresh):
        for j in range(dets // wide):
            height = (j + 1) * wide
            panel = jnp.dot(
                flipped[:height, first:last],
                bits[first:last, j * wide : (j + 1) * wide],
                preferred_element_type=jnp.float32,
            )
            for h in range(2):
                span = slice((2 * j + h) * dets, (2 * j + h) * dets + height)
                part = panel[:, h * PB : (h + 1) * PB]
                grams[span, :] = part if fresh else grams[span, :] + part

    for i in range(chunks):
        copies[i].wait()
        span = slice(i * step, (i + 1) * step)
        values = raw[span, :].astype(jnp.float32)
        counts += jnp.sum(values, axis=0, keepdims=True)
        narrow = values.astype(jnp.bfloat16)
        bits[span, :] = narrow
        flipped[:, span] = narrow.T
        picked = jnp.dot(narrow, picker[...], preferred_element_type=jnp.float32)
        a, b, c = (picked[:, m * triple_count : (m + 1) * triple_count] for m in range(3))
        ab = a * b
        terms = (ab, a * c, b * c, ab * c, a, b, c)
        sums = [s + jnp.sum(t, axis=0, keepdims=True) for s, t in zip(sums, terms, strict=True)]
        if i == chunks // 2 - 1:
            add_grams(0, shots // 2, True)
    add_grams(shots // 2, shots, False)
    part = far * rows_own + vector_rows
    lines = [counts[:, p * PB : (p + 1) * PB] for p in range(patches)]
    lines += [s[:, h * PB : (h + 1) * PB] for s in sums for h in range(halves)]
    lines += [jnp.zeros((1, PB), jnp.float32)] * (vector_rows - len(lines))
    vectors = jnp.concatenate(lines, axis=0)
    for target in (keep, send):
        for x in range(near):
            target[(x + 1) * part - vector_rows : (x + 1) * part, :] = vectors
    mine = core[0]

    def place(block, start):
        for target, side in ((keep, mine), (send, 1 - mine)):
            for x in range(near):
                for r in range(2):
                    rows = grams[pl.ds(start + 4 * far * x + 2 * side + r, far, stride=4), :]
                    target[pl.ds(x * part + 2 * block + r, far, stride=rows_own), :] = rows

    for p in range(patches):
        place(p, p * dets + p * PB)

    def pair(k, carry):
        low, high = ordered(pairs, k)
        place(patches + k, high * dets + low * PB)
        return carry

    lax.fori_loop(0, pair_count, pair, 0)


def route_kernel(
    shot, pairs, owners, own, outgoing, filled, left, right, rates,
    *, patches, pair_count, shot_count, inverse,
):
    rows_own = 2 * (patches + pair_count)
    outgoing[...] = jnp.zeros_like(outgoing)
    for o in range(shot_count):
        filled[o] = 0
    first = 2 * shot[0]
    lane = iota((patches, PB), 1)
    counts = own[rows_own : rows_own + patches, :]
    for r in range(2):
        mine = jnp.sum(jnp.where(lane == first + r, counts, 0.0), axis=1, keepdims=True)
        rates[pl.ds(r * patches, patches), :] = jnp.broadcast_to(mine, (patches, PB))
    for k in range(pair_count):
        low, high = ordered(pairs, k)
        cols = own[pl.ds(rows_own + high, 1), :]
        for r in range(2):
            left[2 * k + r : 2 * k + r + 1, :] = rates[pl.ds(r * patches + low, 1), :]
            right[2 * k + r : 2 * k + r + 1, :] = cols
    rates[...] = fit(own[pl.ds(2 * patches, 2 * pair_count), :], left[...], right[...], inverse)

    def entry(k, carry):
        for m in range(2):
            owner = owners[m, k]
            slot = filled[owner]
            filled[owner] = slot + 1
            for r in range(2):
                outgoing[pl.ds(4 * owner + 2 * slot + r, 1), :] = rates[pl.ds(2 * k + r, 1), :]
        return carry

    lax.fori_loop(0, pair_count, entry, 0)


def intra_kernel(shot, panel, own, rates, loads, cumulant, *, patches, rows_own, inverse):
    vectors = own[rows_own:, :]
    first = 2 * shot[0]
    lines = 2 * patches
    lane = iota((lines, PB), 1)
    line = iota((lines, PB), 0)
    cols = jnp.concatenate([vectors[n // 2 : n // 2 + 1, :] for n in range(lines)], axis=0)
    mine = jnp.sum(jnp.where(lane == first + line % 2, cols, 0.0), axis=1, keepdims=True)
    rate = fit(own[:lines, :], mine, cols, inverse)
    rates[...] = rate
    here = lane == (line % 2) * (PB // 2) + panel[0] * patches + line // 2
    sums = jnp.sum(rate, axis=1, keepdims=True)
    loads[...] = jnp.sum(jnp.where(here, sums, 0.0), axis=0, keepdims=True)
    halves = cumulant.shape[1] // PB
    for h in range(halves):
        ij, il, jl, ijl, i, j, l = (
            vectors[patches + m * halves + h : patches + m * halves + h + 1, :] * inverse for m in range(7)
        )
        kappa = ijl - ij * l - il * j - jl * i + 2.0 * i * j * l
        cumulant[:, h * PB : (h + 1) * PB] = 1000.0 * kappa


def owner_kernel(shot, pairs, owners, arrived, boundary, *, shot_count):
    me = shot[0]
    turns = [jnp.int32(0), jnp.int32(0)]
    held = jnp.int32(0)
    for k in range(pairs.shape[1]):
        turn = (pairs[0, k] > pairs[1, k]).astype(jnp.int32)
        for m in range(2):
            hit = owners[m, k] == me
            turns = [jnp.where(hit & (held == slot), turn, t) for slot, t in enumerate(turns)]
            held = held + hit.astype(jnp.int32)
    for slot in range(2):
        span = pl.ds(slot * PB, PB)
        for r in range(2):
            boundary[pl.ds(slot * PB + r, shot_count, stride=2), :] = arrived[
                pl.ds(2 * slot + r, shot_count, stride=4), :
            ]

        @pl.when(turns[slot] == 1)
        def _():
            boundary[span, :] = boundary[span, :].T


def smem():
    return pl.BlockSpec(memory_space=pltpu.SMEM)


def vmem():
    return pl.BlockSpec(memory_space=pltpu.VMEM)


def f32(*shape):
    return jax.ShapeDtypeStruct(shape, jnp.float32)


def near_f32(*shape):
    return pltpu.VMEM(shape, jnp.float32)


def exchange(x, axis):
    return lax.all_to_all(x, axis, split_axis=0, concat_axis=0, tiled=True)


def local(events, pair_patches, pair_owners, triples, *, interpret=False):
    shot_dev, det_dev = events.shape
    shot_count = lax.axis_size(SHOT)
    det_count = lax.axis_size("det")
    shot = lax.axis_index(SHOT).astype(jnp.int32).reshape(1)
    panel = lax.axis_index("det").astype(jnp.int32).reshape(1)
    core = lax.axis_index(SHOT[2]).astype(jnp.int32).reshape(1)
    inverse = 1.0 / float(shot_dev * shot_count)
    patches = det_dev // PB
    near = lax.axis_size(SHOT[0])
    far = lax.axis_size(SHOT[1])
    pairs = pair_patches[0].T
    pair_count = pairs.shape[1]
    owners = pair_owners[0].T
    triple_rows = triples.transpose(2, 0, 1)
    triple_count = triple_rows.shape[2]
    rows_own = 2 * (patches + pair_count)
    vector_rows = 24
    part = far * rows_own + vector_rows
    own_rows = rows_own + vector_rows
    chunks = 4

    keep, send = pl.pallas_call(
        functools.partial(
            count_kernel,
            chunks=chunks,
            patches=patches,
            pair_count=pair_count,
            near=near,
            far=far,
            rows_own=rows_own,
            vector_rows=vector_rows,
        ),
        out_shape=(near_f32(near * part, PB), near_f32(near * part, PB)),
        in_specs=[smem(), smem(), vmem(), pl.BlockSpec(memory_space=pl.ANY)],
        out_specs=(vmem(), vmem()),
        scratch_shapes=[
            pltpu.VMEM((shot_dev, det_dev), jnp.int32),
            pltpu.VMEM((shot_dev, det_dev), jnp.bfloat16),
            pltpu.VMEM((det_dev, shot_dev), jnp.bfloat16),
            pltpu.VMEM((patches * det_dev, PB), jnp.float32),
            pltpu.VMEM((det_dev, 3 * triple_count), jnp.bfloat16),
            pltpu.SemaphoreType.DMA((chunks,)),
        ],
        interpret=interpret,
        name="count",
    )(core, pairs, triple_rows, events)
    other = lax.ppermute(send, SHOT[2], [(0, 1), (1, 0)])
    half = keep + other
    arrived = exchange(half.reshape(near, part, PB), SHOT[0])
    total = arrived.sum(axis=0)
    grams = total[: far * rows_own].reshape(far, rows_own // 4, 4, PB)
    vector = total[far * rows_own :].reshape(1, vector_rows // 4, 4, PB)
    vector = jnp.broadcast_to(vector, (far, *vector.shape[1:]))
    vector = jnp.pad(vector, ((0, 0), (0, (-own_rows % 8) // 4), (0, 0), (0, 0)))
    arrived = exchange(jnp.concatenate([grams, vector], axis=1), SHOT[1])
    own = pltpu.with_memory_space_constraint(arrived.sum(axis=0).reshape(-1, PB), pltpu.VMEM)
    outgoing = pl.pallas_call(
        functools.partial(
            route_kernel,
            patches=patches,
            pair_count=pair_count,
            shot_count=shot_count,
            inverse=inverse,
        ),
        out_shape=near_f32(shot_count * 4, PB),
        in_specs=[smem(), smem(), smem(), vmem()],
        out_specs=vmem(),
        scratch_shapes=[
            pltpu.SMEM((shot_count,), jnp.int32),
            pltpu.VMEM((2 * pair_count, PB), jnp.float32),
            pltpu.VMEM((2 * pair_count, PB), jnp.float32),
            pltpu.VMEM((2 * pair_count, PB), jnp.float32),
        ],
        interpret=interpret,
        name="route",
    )(shot, pairs, owners, own)
    incoming = exchange(outgoing.reshape(shot_count, 4, PB), SHOT)
    rates, loads, cumulant = pl.pallas_call(
        functools.partial(intra_kernel, patches=patches, rows_own=rows_own, inverse=inverse),
        out_shape=(f32(2 * patches, PB), near_f32(1, PB), f32(1, triple_count)),
        in_specs=[smem(), smem(), vmem()],
        out_specs=(vmem(), vmem(), vmem()),
        interpret=interpret,
        name="intra",
    )(shot, panel, own)
    load = lax.all_gather(loads, "det").sum(axis=0)
    detector_load = load.reshape(2, det_count * patches).T
    incoming = pltpu.with_memory_space_constraint(incoming.reshape(4 * shot_count, PB), pltpu.VMEM)
    boundary = pl.pallas_call(
        functools.partial(owner_kernel, shot_count=shot_count),
        out_shape=f32(2 * PB, PB),
        in_specs=[smem(), smem(), smem(), vmem()],
        out_specs=vmem(),
        interpret=interpret,
        name="owner",
    )(shot, pairs, owners, incoming)
    return (
        rates.reshape(patches, 2, PB),
        boundary.reshape(1, 1, 2, PB, PB),
        detector_load,
        cumulant,
    )


def solution(mesh):
    torus = Mesh(
        mesh.devices.reshape(4, 8, 2, mesh.shape["det"]), ("shot_0", "shot_1", "shot_2", "det")
    )
    return jax.shard_map(
        local,
        mesh=torus,
        in_specs=(P(SHOT, "det"), P("det", None, None), P("det", None, None), P("det", None, None)),
        out_specs=(
            P("det", SHOT, None),
            P("det", SHOT, None, None, None),
            P(None, SHOT),
            P("det", None),
        ),
        check_vma=False,
    )
```

```python
import functools

import jax
import jax.numpy as jnp
from jax import lax
from jax.experimental import pallas as pl
from jax.experimental.pallas import tpu as pltpu
from jax.sharding import Mesh
from jax.sharding import PartitionSpec as P

PB = 128
SHOT = ("shot_0", "shot_1", "shot_2")
SLOT_ROWS = 8


def fit(joint, rows, cols, inverse):
    u = joint * inverse
    x = rows * inverse
    y = cols * inverse
    den = jnp.maximum(1.0 - 2.0 * x - 2.0 * y + 4.0 * u, 0.25)
    q = (u - x * y) / den
    return 100.0 * (0.5 - 0.5 * jnp.sqrt(jnp.maximum(1.0 - 4.0 * q, 0.04)))


def iota(shape, dim):
    return lax.broadcasted_iota(jnp.int32, shape, dim)


def ordered(pairs, k):
    return jnp.minimum(pairs[0, k], pairs[1, k]), jnp.maximum(pairs[0, k], pairs[1, k])


def table_kernel(shot, panel, pairs, owners, table, filled, *, shot_count):
    table[6, 0] = shot[0]
    table[6, 1] = panel[0]

    def clear(o, carry):
        filled[o] = 0
        return carry

    lax.fori_loop(0, shot_count, clear, 0)

    def pair(k, carry):
        for m in range(2):
            owner = owners[m, k]
            slot = filled[owner]
            filled[owner] = slot + 1
            table[m, k] = owner * SLOT_ROWS + 2 * slot
            table[2 + m, k] = owner * SLOT_ROWS + 5 + slot
        low, high = ordered(pairs, k)
        table[4, k] = low
        table[5, k] = high
        table[7, k] = (pairs[0, k] > pairs[1, k]).astype(jnp.int32)
        return carry

    lax.fori_loop(0, pairs.shape[1], pair, 0)


def count_kernel(
    shot_in, pairs_in, triples_in, events, keep, send,
    raw, bits, flipped, grams, picker, shot, pairs, triple_rows, small, sems,
    *, chunks, patches, pair_count, near, far, rows_own,
):
    shots, dets = raw.shape
    step = shots // chunks
    triple_count = triple_rows.shape[2]
    copies = [
        pltpu.make_async_copy(events.at[pl.ds(i * step, step)], raw.at[pl.ds(i * step, step)], sems.at[i])
        for i in range(chunks)
    ]
    few = [
        pltpu.make_async_copy(source, target, small.at[i])
        for i, (source, target) in enumerate(((triples_in, triple_rows), (pairs_in, pairs), (shot_in, shot)))
    ]
    few[0].start()
    for copy in (*copies, *few[1:]):
        copy.start()
    few[0].wait()
    detector = iota((dets, triple_count), 0)
    for m in range(3):
        hit = detector == triple_rows[m]
        picker[:, m * triple_count : (m + 1) * triple_count] = jnp.where(hit, 1.0, 0.0).astype(jnp.float8_e4m3fn)
    counts = jnp.zeros((1, dets), jnp.float32)
    sums = [jnp.zeros((1, triple_count), jnp.float32) for _ in range(7)]
    wide = 2 * PB

    def add_grams(first, last, fresh):
        for j in range(dets // wide):
            height = (j + 1) * wide
            panel = jnp.dot(
                flipped[:height, first:last],
                bits[first:last, j * wide : (j + 1) * wide],
                preferred_element_type=jnp.float32,
            )
            for h in range(2):
                span = slice((2 * j + h) * dets, (2 * j + h) * dets + height)
                part = panel[:, h * PB : (h + 1) * PB]
                grams[span, :] = part if fresh else grams[span, :] + part

    for i in range(chunks):
        copies[i].wait()
        span = slice(i * step, (i + 1) * step)
        values = raw[span, :].astype(jnp.float32)
        counts += jnp.sum(values, axis=0, keepdims=True)
        narrow = values.astype(jnp.bfloat16)
        bits[span, :] = narrow
        flipped[:, span] = narrow.T
        picked = jnp.dot(values.astype(jnp.float8_e4m3fn), picker[...], preferred_element_type=jnp.float32)
        a, b, c = (picked[:, m * triple_count : (m + 1) * triple_count] for m in range(3))
        ab = a * b
        terms = (ab, a * c, b * c, ab * c, a, b, c)
        sums = [s + jnp.sum(t, axis=0, keepdims=True) for s, t in zip(sums, terms, strict=True)]
        if i == chunks // 2 - 1:
            add_grams(0, shots // 2, True)
    add_grams(shots // 2, shots, False)
    part = far * rows_own + patches
    group = triple_count // far
    zeros = jnp.zeros((far, PB), jnp.float32)
    lines = []
    for n in range(0, len(sums), PB // group):
        members = sums[n : n + PB // group]
        members += [jnp.zeros((1, triple_count), jnp.float32)] * (PB // group - len(members))
        rows = [
            jnp.concatenate([t[:, y * group : (y + 1) * group] for t in members], axis=1) for y in range(far)
        ]
        lines.append(jnp.concatenate(rows, axis=0))
    lines += [zeros] * (rows_own - 2 * (patches + pair_count) - len(lines))
    for target in (keep, send):
        for x in range(near):
            for n, line in enumerate(lines):
                row = x * part + 2 * (patches + pair_count) + n
                target[pl.ds(row, far, stride=rows_own), :] = line
            for p in range(patches):
                row = (x + 1) * part - patches + p
                target[row : row + 1, :] = counts[:, p * PB : (p + 1) * PB]
    few[1].wait()
    few[2].wait()
    mine = shot[0] % 2

    def place(block, start):
        for target, side in ((keep, mine), (send, 1 - mine)):
            for x in range(near):
                for r in range(2):
                    rows = grams[pl.ds(start + 4 * far * x + 2 * side + r, far, stride=4), :]
                    target[pl.ds(x * part + 2 * block + r, far, stride=rows_own), :] = rows

    for p in range(patches):
        place(p, p * dets + p * PB)

    def pair(k, carry):
        low, high = ordered(pairs, k)
        place(patches + k, high * dets + low * PB)
        return carry

    lax.fori_loop(0, pair_count, pair, 0)


def fold_kernel(arrived, payload, *, near, far, rows_own, patches):
    part = far * rows_own + patches

    def total(start, rows):
        value = arrived[start : start + rows, :]
        for x in range(1, near):
            value += arrived[x * part + start : x * part + start + rows, :]
        return value

    counts = total(far * rows_own, patches)
    for y in range(far):
        row = y * (rows_own + patches)
        payload[row : row + rows_own, :] = total(y * rows_own, rows_own)
        payload[row + rows_own : row + rows_own + patches, :] = counts


def route_kernel(
    table, arrived, outgoing, intra, loads, own, left, right, rates,
    *, patches, pair_count, far, group, inverse,
):
    total = arrived[0]
    for y in range(1, far):
        total += arrived[y]
    own[...] = total
    vector_row = 2 * (patches + pair_count)
    counts_row = total.shape[0] - patches
    first = 2 * table[6, 0]
    lines = 2 * patches
    lane = iota((lines, PB), 1)
    line = iota((lines, PB), 0)
    counts = own[counts_row:, :]
    both = jnp.concatenate([counts, counts], axis=0)
    mine = jnp.sum(jnp.where(lane == first + line // patches, both, 0.0), axis=1, keepdims=True)
    rates[:lines, :] = jnp.broadcast_to(mine, (lines, PB))
    for k in range(pair_count):
        low, high = table[4, k], table[5, k]
        cols = own[pl.ds(counts_row + high, 1), :]
        for r in range(2):
            left[2 * k + r : 2 * k + r + 1, :] = rates[pl.ds(r * patches + low, 1), :]
            right[2 * k + r : 2 * k + r + 1, :] = cols
    rates[...] = fit(own[lines : lines + 2 * pair_count, :], left[...], right[...], inverse)
    terms = []
    for n in range(7):
        row = vector_row + n * group // PB
        at = n * group % PB
        terms.append(own[row : row + 1, at : at + group] * inverse)
    ij, il, jl, ijl, i, j, l = terms
    kappa = ijl - ij * l - il * j - jl * i + 2.0 * i * j * l
    kappa = jnp.concatenate([1000.0 * kappa, jnp.zeros((1, PB - group), jnp.float32)], axis=1)
    base = jnp.where(iota((SLOT_ROWS, PB), 0) == 4, kappa, 0.0)
    for o in range(outgoing.shape[0] // SLOT_ROWS):
        outgoing[o * SLOT_ROWS : (o + 1) * SLOT_ROWS, :] = base
    for k in range(pair_count):
        turned = jnp.full((1, PB), table[7, k].astype(jnp.float32), jnp.float32)
        for m in range(2):
            at = table[m, k]
            outgoing[pl.ds(table[2 + m, k], 1), :] = turned
            for r in range(2):
                outgoing[pl.ds(at + r, 1), :] = rates[2 * k + r : 2 * k + r + 1, :]
    cols = jnp.concatenate([counts[n // 2 : n // 2 + 1, :] for n in range(lines)], axis=0)
    mine = jnp.sum(jnp.where(lane == first + line % 2, cols, 0.0), axis=1, keepdims=True)
    rate = fit(own[:lines, :], mine, cols, inverse)
    intra[...] = rate
    here = lane == (line % 2) * (PB // 2) + table[6, 1] * patches + line // 2
    sums = jnp.sum(rate, axis=1, keepdims=True)
    loads[...] = jnp.sum(jnp.where(here, sums, 0.0), axis=0, keepdims=True)


def owner_kernel(panels, arrived, boundary, loads, cumulant, *, shot_count, far, group):
    for slot in range(2):
        span = pl.ds(slot * PB, PB)
        for r in range(2):
            boundary[pl.ds(slot * PB + r, shot_count, stride=2), :] = arrived[
                pl.ds(2 * slot + r, shot_count, stride=SLOT_ROWS), :
            ]
        straight = boundary[span, :]
        turned = arrived[5 + slot : 6 + slot, :] > 0.5
        boundary[span, :] = jnp.where(turned, straight.T, straight)
    load = jnp.sum(panels[...], axis=0, keepdims=True)
    half = PB // 2
    loads[...] = jnp.concatenate([load[:, :half], load[:, half:]], axis=0)
    for y in range(far):
        row = 2 * y * SLOT_ROWS + 4
        cumulant[:, y * group : (y + 1) * group] = arrived[row : row + 1, :group]


def smem():
    return pl.BlockSpec(memory_space=pltpu.SMEM)


def vmem():
    return pl.BlockSpec(memory_space=pltpu.VMEM)


def f32(*shape):
    return jax.ShapeDtypeStruct(shape, jnp.float32)


def near_f32(*shape):
    return pltpu.VMEM(shape, jnp.float32)


def within(x):
    return pltpu.with_memory_space_constraint(x, pltpu.VMEM)


def exchange(x, axis):
    return lax.all_to_all(x, axis, split_axis=0, concat_axis=0, tiled=True)


def local(events, pair_patches, pair_owners, triples, *, interpret=False):
    shot_dev, det_dev = events.shape
    shot_count = lax.axis_size(SHOT)
    det_count = lax.axis_size("det")
    shot = lax.axis_index(SHOT).astype(jnp.int32).reshape(1)
    panel = lax.axis_index("det").astype(jnp.int32).reshape(1)
    inverse = 1.0 / float(shot_dev * shot_count)
    patches = det_dev // PB
    near = lax.axis_size(SHOT[0])
    far = lax.axis_size(SHOT[1])
    pairs = pair_patches[0].T
    pair_count = pairs.shape[1]
    owners = pair_owners[0].T
    triple_rows = triples.transpose(2, 0, 1)
    triple_count = triple_rows.shape[2]
    group = triple_count // far
    rows_own = 2 * (patches + pair_count) + 4
    own_rows = rows_own + patches
    part = far * rows_own + patches
    chunks = 4

    keep, send = pl.pallas_call(
        functools.partial(
            count_kernel,
            chunks=chunks,
            patches=patches,
            pair_count=pair_count,
            near=near,
            far=far,
            rows_own=rows_own,
        ),
        out_shape=(near_f32(near * part, PB), near_f32(near * part, PB)),
        in_specs=[pl.BlockSpec(memory_space=pl.ANY)] * 4,
        out_specs=(vmem(), vmem()),
        scratch_shapes=[
            pltpu.VMEM((shot_dev, det_dev), jnp.int32),
            pltpu.VMEM((shot_dev, det_dev), jnp.bfloat16),
            pltpu.VMEM((det_dev, shot_dev), jnp.bfloat16),
            pltpu.VMEM((patches * det_dev, PB), jnp.float32),
            pltpu.VMEM((det_dev, 3 * triple_count), jnp.float8_e4m3fn),
            pltpu.SMEM((1,), jnp.int32),
            pltpu.SMEM((2, pair_count), jnp.int32),
            pltpu.VMEM((3, 1, triple_count), jnp.int32),
            pltpu.SemaphoreType.DMA((3,)),
            pltpu.SemaphoreType.DMA((chunks,)),
        ],
        interpret=interpret,
        name="count",
    )(shot, pairs, triple_rows, events)
    late_pairs, late_owners, _ = lax.optimization_barrier((pairs, owners, send))
    table = pl.pallas_call(
        functools.partial(table_kernel, shot_count=shot_count),
        out_shape=jax.ShapeDtypeStruct((8, pair_count), jnp.int32),
        in_specs=[smem()] * 4,
        out_specs=smem(),
        scratch_shapes=[pltpu.SMEM((shot_count,), jnp.int32)],
        interpret=interpret,
        name="table",
    )(shot, panel, late_pairs, late_owners)
    other = lax.ppermute(send, SHOT[2], [(0, 1), (1, 0)])
    half = keep + other
    arrived = exchange(half.reshape(near, part, PB), SHOT[0])
    payload = pl.pallas_call(
        functools.partial(fold_kernel, near=near, far=far, rows_own=rows_own, patches=patches),
        out_shape=near_f32(far * own_rows, PB),
        in_specs=[vmem()],
        out_specs=vmem(),
        interpret=interpret,
        name="fold",
    )(within(arrived.reshape(near * part, PB)))
    arrived = exchange(payload.reshape(far, own_rows, PB), SHOT[1])
    outgoing, rates, loads = pl.pallas_call(
        functools.partial(
            route_kernel, patches=patches, pair_count=pair_count, far=far, group=group, inverse=inverse
        ),
        out_shape=(near_f32(shot_count * SLOT_ROWS, PB), f32(2 * patches, PB), near_f32(1, PB)),
        in_specs=[smem(), vmem()],
        out_specs=(vmem(), vmem(), vmem()),
        scratch_shapes=[
            pltpu.VMEM((own_rows, PB), jnp.float32),
            pltpu.VMEM((2 * pair_count, PB), jnp.float32),
            pltpu.VMEM((2 * pair_count, PB), jnp.float32),
            pltpu.VMEM((2 * pair_count, PB), jnp.float32),
        ],
        interpret=interpret,
        name="route",
    )(table, within(arrived))
    incoming = exchange(outgoing.reshape(shot_count, SLOT_ROWS, PB), SHOT)
    panels = lax.all_gather(loads, "det").reshape(det_count, PB)
    boundary, load, cumulant = pl.pallas_call(
        functools.partial(owner_kernel, shot_count=shot_count, far=far, group=group),
        out_shape=(f32(2 * PB, PB), f32(2, det_count * patches), f32(1, triple_count)),
        in_specs=[vmem(), vmem()],
        out_specs=(vmem(), vmem(), vmem()),
        interpret=interpret,
        name="owner",
    )(within(panels), within(incoming.reshape(SLOT_ROWS * shot_count, PB)))
    return (
        rates.reshape(patches, 2, PB),
        boundary.reshape(1, 1, 2, PB, PB),
        load.T,
        cumulant,
    )


def solution(mesh):
    torus = Mesh(
        mesh.devices.reshape(4, 8, 2, mesh.shape["det"]), ("shot_0", "shot_1", "shot_2", "det")
    )
    return jax.shard_map(
        local,
        mesh=torus,
        in_specs=(P(SHOT, "det"), P("det", None, None), P("det", None, None), P("det", None, None)),
        out_specs=(
            P("det", SHOT, None),
            P("det", SHOT, None, None, None),
            P(None, SHOT),
            P("det", None),
        ),
        check_vma=False,
    )
```

```python
import functools

import jax
import jax.numpy as jnp
from jax import lax
from jax.experimental import pallas as pl
from jax.experimental.pallas import tpu as pltpu
from jax.sharding import Mesh
from jax.sharding import PartitionSpec as P

PB = 128
SHOT = ("shot_0", "shot_1", "shot_2")
SLOT_ROWS = 8


def fit(joint, rows, cols, inverse):
    u = joint * inverse
    x = rows * inverse
    y = cols * inverse
    den = jnp.maximum(1.0 - 2.0 * x - 2.0 * y + 4.0 * u, 0.25)
    q = (u - x * y) / den
    return 100.0 * (0.5 - 0.5 * jnp.sqrt(jnp.maximum(1.0 - 4.0 * q, 0.04)))


def iota(shape, dim):
    return lax.broadcasted_iota(jnp.int32, shape, dim)


def ordered(pairs, k):
    return jnp.minimum(pairs[0, k], pairs[1, k]), jnp.maximum(pairs[0, k], pairs[1, k])


def fill_table(shot, panel, pairs, owners, table, filled):
    for n in range(pairs.shape[1]):
        table[6, n] = shot[0] if n == 0 else panel[0]
    for o in range(filled.shape[0]):
        filled[o] = 0
    for k in range(pairs.shape[1]):
        for m in range(2):
            owner = owners[m, k]
            slot = filled[owner]
            filled[owner] = slot + 1
            table[m, k] = owner * SLOT_ROWS + 2 * slot
            table[2 + m, k] = owner * SLOT_ROWS + 5 + slot
        low, high = ordered(pairs, k)
        table[4, k] = low
        table[5, k] = high
        table[7, k] = (pairs[0, k] > pairs[1, k]).astype(jnp.int32)


def count_kernel(
    shot_in, panel_in, pairs_in, owners_in, triples_in, events, keep, send, table_out,
    raw, bits, flipped, grams, picker, shot, panel, pairs, owners, table, filled, triple_rows, small, sems,
    *, chunks, patches, pair_count, near, far, rows_own,
):
    shots, dets = raw.shape
    step = shots // chunks
    triple_count = triple_rows.shape[2]
    copies = [
        pltpu.make_async_copy(events.at[pl.ds(i * step, step)], raw.at[pl.ds(i * step, step)], sems.at[i])
        for i in range(chunks)
    ]
    given = (
        (triples_in, triple_rows),
        (pairs_in, pairs),
        (owners_in, owners),
        (shot_in, shot),
        (panel_in, panel),
    )
    few = [pltpu.make_async_copy(source, target, small.at[i]) for i, (source, target) in enumerate(given)]
    copy_table = pltpu.make_async_copy(table, table_out, small.at[len(few)])
    for copy in (*few, *copies):
        copy.start()
    for copy in few:
        copy.wait()
    fill_table(shot, panel, pairs, owners, table, filled)
    detector = iota((dets, triple_count), 0)
    for m in range(3):
        hit = detector == triple_rows[m]
        picker[:, m * triple_count : (m + 1) * triple_count] = jnp.where(hit, 1.0, 0.0).astype(jnp.float8_e4m3fn)
    copy_table.start()
    counts = jnp.zeros((1, dets), jnp.float32)
    sums = [jnp.zeros((1, triple_count), jnp.float32) for _ in range(7)]
    wide = 2 * PB

    def add_grams(first, last, fresh):
        for j in range(dets // wide):
            height = (j + 1) * wide
            panel = jnp.dot(
                flipped[:height, first:last],
                bits[first:last, j * wide : (j + 1) * wide],
                preferred_element_type=jnp.float32,
            )
            for h in range(2):
                span = slice((2 * j + h) * dets, (2 * j + h) * dets + height)
                part = panel[:, h * PB : (h + 1) * PB]
                grams[span, :] = part if fresh else grams[span, :] + part

    for i in range(chunks):
        copies[i].wait()
        span = slice(i * step, (i + 1) * step)
        values = raw[span, :].astype(jnp.float32)
        counts += jnp.sum(values, axis=0, keepdims=True)
        narrow = values.astype(jnp.bfloat16)
        bits[span, :] = narrow
        flipped[:, span] = narrow.T
        picked = jnp.dot(values.astype(jnp.float8_e4m3fn), picker[...], preferred_element_type=jnp.float32)
        a, b, c = (picked[:, m * triple_count : (m + 1) * triple_count] for m in range(3))
        ab = a * b
        terms = (ab, a * c, b * c, ab * c, a, b, c)
        sums = [s + jnp.sum(t, axis=0, keepdims=True) for s, t in zip(sums, terms, strict=True)]
        if i == chunks // 2 - 1:
            add_grams(0, shots // 2, True)
    add_grams(shots // 2, shots, False)
    part = far * rows_own + patches
    group = triple_count // far
    zeros = jnp.zeros((far, PB), jnp.float32)
    lines = []
    for n in range(0, len(sums), PB // group):
        members = sums[n : n + PB // group]
        members += [jnp.zeros((1, triple_count), jnp.float32)] * (PB // group - len(members))
        rows = [
            jnp.concatenate([t[:, y * group : (y + 1) * group] for t in members], axis=1) for y in range(far)
        ]
        lines.append(jnp.concatenate(rows, axis=0))
    lines += [zeros] * (rows_own - 2 * (patches + pair_count) - len(lines))
    for target in (keep, send):
        for x in range(near):
            for n, line in enumerate(lines):
                row = x * part + 2 * (patches + pair_count) + n
                target[pl.ds(row, far, stride=rows_own), :] = line
            for p in range(patches):
                row = (x + 1) * part - patches + p
                target[row : row + 1, :] = counts[:, p * PB : (p + 1) * PB]
    mine = shot[0] % 2

    def place(block, start):
        for target, side in ((keep, mine), (send, 1 - mine)):
            for x in range(near):
                for r in range(2):
                    rows = grams[pl.ds(start + 4 * far * x + 2 * side + r, far, stride=4), :]
                    target[pl.ds(x * part + 2 * block + r, far, stride=rows_own), :] = rows

    for p in range(patches):
        place(p, p * dets + p * PB)

    for k in range(pair_count):
        place(patches + k, table[5, k] * dets + table[4, k] * PB)
    copy_table.wait()


def fold_kernel(arrived, payload, *, near, far, rows_own, patches):
    part = far * rows_own + patches

    def total(start, rows):
        value = arrived[start : start + rows, :]
        for x in range(1, near):
            value += arrived[x * part + start : x * part + start + rows, :]
        return value

    counts = total(far * rows_own, patches)
    for y in range(far):
        row = y * (rows_own + patches)
        payload[row : row + rows_own, :] = total(y * rows_own, rows_own)
        payload[row + rows_own : row + rows_own + patches, :] = counts


def route_kernel(
    table, arrived, outgoing, intra, loads, own, left, right, rates,
    *, patches, pair_count, far, group, inverse,
):
    total = arrived[0]
    for y in range(1, far):
        total += arrived[y]
    own[...] = total
    vector_row = 2 * (patches + pair_count)
    counts_row = total.shape[0] - patches
    first = 2 * table[6, 0]
    lines = 2 * patches
    lane = iota((lines, PB), 1)
    line = iota((lines, PB), 0)
    counts = own[counts_row:, :]
    both = jnp.concatenate([counts, counts], axis=0)
    mine = jnp.sum(jnp.where(lane == first + line // patches, both, 0.0), axis=1, keepdims=True)
    rates[:lines, :] = jnp.broadcast_to(mine, (lines, PB))
    for k in range(pair_count):
        low, high = table[4, k], table[5, k]
        cols = own[pl.ds(counts_row + high, 1), :]
        for r in range(2):
            left[2 * k + r : 2 * k + r + 1, :] = rates[pl.ds(r * patches + low, 1), :]
            right[2 * k + r : 2 * k + r + 1, :] = cols
    rates[...] = fit(own[lines : lines + 2 * pair_count, :], left[...], right[...], inverse)
    terms = []
    for n in range(7):
        row = vector_row + n * group // PB
        at = n * group % PB
        terms.append(own[row : row + 1, at : at + group] * inverse)
    ij, il, jl, ijl, i, j, l = terms
    kappa = ijl - ij * l - il * j - jl * i + 2.0 * i * j * l
    kappa = jnp.concatenate([1000.0 * kappa, jnp.zeros((1, PB - group), jnp.float32)], axis=1)
    base = jnp.where(iota((SLOT_ROWS, PB), 0) == 4, kappa, 0.0)
    for o in range(outgoing.shape[0] // SLOT_ROWS):
        outgoing[o * SLOT_ROWS : (o + 1) * SLOT_ROWS, :] = base
    for k in range(pair_count):
        turned = jnp.full((1, PB), table[7, k].astype(jnp.float32), jnp.float32)
        for m in range(2):
            at = table[m, k]
            outgoing[pl.ds(table[2 + m, k], 1), :] = turned
            for r in range(2):
                outgoing[pl.ds(at + r, 1), :] = rates[2 * k + r : 2 * k + r + 1, :]
    cols = jnp.concatenate([counts[n // 2 : n // 2 + 1, :] for n in range(lines)], axis=0)
    mine = jnp.sum(jnp.where(lane == first + line % 2, cols, 0.0), axis=1, keepdims=True)
    rate = fit(own[:lines, :], mine, cols, inverse)
    intra[...] = rate
    here = lane == (line % 2) * (PB // 2) + table[6, 1] * patches + line // 2
    sums = jnp.sum(rate, axis=1, keepdims=True)
    loads[...] = jnp.sum(jnp.where(here, sums, 0.0), axis=0, keepdims=True)


def owner_kernel(panels, arrived, boundary, loads, cumulant, *, shot_count, far, group):
    for slot in range(2):
        span = pl.ds(slot * PB, PB)
        for r in range(2):
            boundary[pl.ds(slot * PB + r, shot_count, stride=2), :] = arrived[
                pl.ds(2 * slot + r, shot_count, stride=SLOT_ROWS), :
            ]
        straight = boundary[span, :]
        turned = arrived[5 + slot : 6 + slot, :] > 0.5
        boundary[span, :] = jnp.where(turned, straight.T, straight)
    load = jnp.sum(panels[...], axis=0, keepdims=True)
    half = PB // 2
    loads[...] = jnp.concatenate([load[:, :half], load[:, half:]], axis=0)
    for y in range(far):
        row = 2 * y * SLOT_ROWS + 4
        cumulant[:, y * group : (y + 1) * group] = arrived[row : row + 1, :group]


def smem():
    return pl.BlockSpec(memory_space=pltpu.SMEM)


def vmem():
    return pl.BlockSpec(memory_space=pltpu.VMEM)


def f32(*shape):
    return jax.ShapeDtypeStruct(shape, jnp.float32)


def near_f32(*shape):
    return pltpu.VMEM(shape, jnp.float32)


def within(x):
    return pltpu.with_memory_space_constraint(x, pltpu.VMEM)


def exchange(x, axis):
    return lax.all_to_all(x, axis, split_axis=0, concat_axis=0, tiled=True)


def local(events, pair_patches, pair_owners, triples, *, interpret=False):
    shot_dev, det_dev = events.shape
    shot_count = lax.axis_size(SHOT)
    det_count = lax.axis_size("det")
    shot = lax.axis_index(SHOT).astype(jnp.int32).reshape(1)
    panel = lax.axis_index("det").astype(jnp.int32).reshape(1)
    inverse = 1.0 / float(shot_dev * shot_count)
    patches = det_dev // PB
    near = lax.axis_size(SHOT[0])
    far = lax.axis_size(SHOT[1])
    pairs = pair_patches[0].T
    pair_count = pairs.shape[1]
    owners = pair_owners[0].T
    triple_rows = triples.transpose(2, 0, 1)
    triple_count = triple_rows.shape[2]
    group = triple_count // far
    rows_own = 2 * (patches + pair_count) + 4
    own_rows = rows_own + patches
    part = far * rows_own + patches
    chunks = 4

    keep, send, table = pl.pallas_call(
        functools.partial(
            count_kernel,
            chunks=chunks,
            patches=patches,
            pair_count=pair_count,
            near=near,
            far=far,
            rows_own=rows_own,
        ),
        out_shape=(
            near_f32(near * part, PB),
            near_f32(near * part, PB),
            jax.ShapeDtypeStruct((8, pair_count), jnp.int32),
        ),
        in_specs=[pl.BlockSpec(memory_space=pl.ANY)] * 6,
        out_specs=(vmem(), vmem(), pl.BlockSpec(memory_space=pl.ANY)),
        scratch_shapes=[
            pltpu.VMEM((shot_dev, det_dev), jnp.int32),
            pltpu.VMEM((shot_dev, det_dev), jnp.bfloat16),
            pltpu.VMEM((det_dev, shot_dev), jnp.bfloat16),
            pltpu.VMEM((patches * det_dev, PB), jnp.float32),
            pltpu.VMEM((det_dev, 3 * triple_count), jnp.float8_e4m3fn),
            pltpu.SMEM((1,), jnp.int32),
            pltpu.SMEM((1,), jnp.int32),
            pltpu.SMEM((2, pair_count), jnp.int32),
            pltpu.SMEM((2, pair_count), jnp.int32),
            pltpu.SMEM((8, pair_count), jnp.int32),
            pltpu.SMEM((shot_count,), jnp.int32),
            pltpu.VMEM((3, 1, triple_count), jnp.int32),
            pltpu.SemaphoreType.DMA((6,)),
            pltpu.SemaphoreType.DMA((chunks,)),
        ],
        interpret=interpret,
        name="count",
    )(shot, panel, pairs, owners, triple_rows, events)
    other = lax.ppermute(send, SHOT[2], [(0, 1), (1, 0)])
    half = keep + other
    arrived = exchange(half.reshape(near, part, PB), SHOT[0])
    payload = pl.pallas_call(
        functools.partial(fold_kernel, near=near, far=far, rows_own=rows_own, patches=patches),
        out_shape=near_f32(far * own_rows, PB),
        in_specs=[vmem()],
        out_specs=vmem(),
        interpret=interpret,
        name="fold",
    )(within(arrived.reshape(near * part, PB)))
    arrived = exchange(payload.reshape(far, own_rows, PB), SHOT[1])
    outgoing, rates, loads = pl.pallas_call(
        functools.partial(route_kernel, patches=patches, pair_count=pair_count, far=far, group=group, inverse=inverse),
        out_shape=(near_f32(shot_count * SLOT_ROWS, PB), f32(2 * patches, PB), near_f32(1, PB)),
        in_specs=[smem(), vmem()],
        out_specs=(vmem(), vmem(), vmem()),
        scratch_shapes=[
            pltpu.VMEM((own_rows, PB), jnp.float32),
            pltpu.VMEM((2 * pair_count, PB), jnp.float32),
            pltpu.VMEM((2 * pair_count, PB), jnp.float32),
            pltpu.VMEM((2 * pair_count, PB), jnp.float32),
        ],
        interpret=interpret,
        name="route",
    )(table, within(arrived))
    incoming = exchange(outgoing.reshape(shot_count, SLOT_ROWS, PB), SHOT)
    panels = lax.all_gather(loads, "det").reshape(det_count, PB)
    boundary, load, cumulant = pl.pallas_call(
        functools.partial(owner_kernel, shot_count=shot_count, far=far, group=group),
        out_shape=(f32(2 * PB, PB), f32(2, det_count * patches), f32(1, triple_count)),
        in_specs=[vmem(), vmem()],
        out_specs=(vmem(), vmem(), vmem()),
        interpret=interpret,
        name="owner",
    )(within(panels), within(incoming.reshape(SLOT_ROWS * shot_count, PB)))
    return (
        rates.reshape(patches, 2, PB),
        boundary.reshape(1, 1, 2, PB, PB),
        load.T,
        cumulant,
    )


def solution(mesh):
    torus = Mesh(
        mesh.devices.reshape(4, 8, 2, mesh.shape["det"]), ("shot_0", "shot_1", "shot_2", "det")
    )
    return jax.shard_map(
        local,
        mesh=torus,
        in_specs=(P(SHOT, "det"), P("det", None, None), P("det", None, None), P("det", None, None)),
        out_specs=(
            P("det", SHOT, None),
            P("det", SHOT, None, None, None),
            P(None, SHOT),
            P("det", None),
        ),
        check_vma=False,
    )
```

```python
import functools

import jax
import jax.numpy as jnp
from jax import lax
from jax.experimental import pallas as pl
from jax.experimental.pallas import tpu as pltpu
from jax.sharding import Mesh
from jax.sharding import PartitionSpec as P

PB = 128
SHOT = ("shot_0", "shot_1", "shot_2")
SLOT_ROWS = 8


def fit(joint, rows, cols, inverse):
    u = joint * inverse
    x = rows * inverse
    y = cols * inverse
    den = jnp.maximum(1.0 - 2.0 * x - 2.0 * y + 4.0 * u, 0.25)
    q = (u - x * y) / den
    return 100.0 * (0.5 - 0.5 * jnp.sqrt(jnp.maximum(1.0 - 4.0 * q, 0.04)))


def iota(shape, dim):
    return lax.broadcasted_iota(jnp.int32, shape, dim)


def ordered(pairs, k):
    return jnp.minimum(pairs[0, k], pairs[1, k]), jnp.maximum(pairs[0, k], pairs[1, k])


def fill_table(shot, panel, pairs, owners, table, filled):
    for n in range(pairs.shape[1]):
        table[6, n] = shot[0] if n == 0 else panel[0]
    for o in range(filled.shape[0]):
        filled[o] = 0
    for k in range(pairs.shape[1]):
        for m in range(2):
            owner = owners[m, k]
            slot = filled[owner]
            filled[owner] = slot + 1
            table[m, k] = owner * SLOT_ROWS + 2 * slot
            table[2 + m, k] = owner * SLOT_ROWS + 5 + slot
        low, high = ordered(pairs, k)
        table[4, k] = low
        table[5, k] = high
        table[7, k] = (pairs[0, k] > pairs[1, k]).astype(jnp.int32)


def count_kernel(
    shot_in, panel_in, pairs_in, owners_in, triples_in, events, keep, send, table_out,
    raw, bits, flipped, grams, picker, shot, panel, pairs, owners, table, filled, triple_rows, small, sems,
    *, chunks, patches, pair_count, near, far, rows_own,
):
    shots, dets = raw.shape
    step = shots // chunks
    triple_count = triple_rows.shape[2]
    copies = [
        pltpu.make_async_copy(events.at[pl.ds(i * step, step)], raw.at[pl.ds(i * step, step)], sems.at[i])
        for i in range(chunks)
    ]
    given = (
        (triples_in, triple_rows),
        (pairs_in, pairs),
        (owners_in, owners),
        (shot_in, shot),
        (panel_in, panel),
    )
    few = [pltpu.make_async_copy(source, target, small.at[i]) for i, (source, target) in enumerate(given)]
    copy_table = pltpu.make_async_copy(table, table_out, small.at[len(few)])
    for copy in (*few, *copies):
        copy.start()
    for copy in few:
        copy.wait()
    fill_table(shot, panel, pairs, owners, table, filled)
    detector = iota((dets, triple_count), 0)
    for m in range(3):
        hit = detector == triple_rows[m]
        picker[:, m * triple_count : (m + 1) * triple_count] = jnp.where(hit, 1.0, 0.0).astype(jnp.float8_e4m3fn)
    copy_table.start()
    counts = jnp.zeros((1, dets), jnp.float32)
    sums = [jnp.zeros((1, triple_count), jnp.float32) for _ in range(7)]
    wide = 2 * PB

    def add_grams(first, last, fresh):
        for j in range(dets // wide):
            height = (j + 1) * wide
            panel = jnp.dot(
                flipped[:height, first:last],
                bits[first:last, j * wide : (j + 1) * wide],
                preferred_element_type=jnp.float32,
            )
            for h in range(2):
                span = slice((2 * j + h) * dets, (2 * j + h) * dets + height)
                part = panel[:, h * PB : (h + 1) * PB]
                grams[span, :] = part if fresh else grams[span, :] + part

    for i in range(chunks):
        copies[i].wait()
        span = slice(i * step, (i + 1) * step)
        values = raw[span, :].astype(jnp.float32)
        counts += jnp.sum(values, axis=0, keepdims=True)
        narrow = values.astype(jnp.bfloat16)
        bits[span, :] = narrow
        flipped[:, span] = narrow.T
        picked = jnp.dot(values.astype(jnp.float8_e4m3fn), picker[...], preferred_element_type=jnp.float32)
        a, b, c = (picked[:, m * triple_count : (m + 1) * triple_count] for m in range(3))
        ab = a * b
        terms = (ab, a * c, b * c, ab * c, a, b, c)
        sums = [s + jnp.sum(t, axis=0, keepdims=True) for s, t in zip(sums, terms, strict=True)]
        if i == chunks // 2 - 1:
            add_grams(0, shots // 2, True)
    add_grams(shots // 2, shots, False)
    part = far * rows_own + patches
    group = triple_count // far
    zeros = jnp.zeros((far, PB), jnp.float32)
    lines = []
    for n in range(0, len(sums), PB // group):
        members = sums[n : n + PB // group]
        members += [jnp.zeros((1, triple_count), jnp.float32)] * (PB // group - len(members))
        rows = [
            jnp.concatenate([t[:, y * group : (y + 1) * group] for t in members], axis=1) for y in range(far)
        ]
        lines.append(jnp.concatenate(rows, axis=0))
    lines += [zeros] * (rows_own - 2 * (patches + pair_count) - len(lines))
    for target in (keep, send):
        for x in range(near):
            for n, line in enumerate(lines):
                row = x * part + 2 * (patches + pair_count) + n
                target[pl.ds(row, far, stride=rows_own), :] = line
            for p in range(patches):
                row = (x + 1) * part - patches + p
                target[row : row + 1, :] = counts[:, p * PB : (p + 1) * PB]
    mine = shot[0] % 2

    def place(block, start):
        for target, side in ((keep, mine), (send, 1 - mine)):
            for x in range(near):
                for r in range(2):
                    rows = grams[pl.ds(start + 4 * far * x + 2 * side + r, far, stride=4), :]
                    target[pl.ds(x * part + 2 * block + r, far, stride=rows_own), :] = rows

    for p in range(patches):
        place(p, p * dets + p * PB)

    for k in range(pair_count):
        place(patches + k, table[5, k] * dets + table[4, k] * PB)
    copy_table.wait()


def fold_kernel(arrived, payload, *, near, far, rows_own, own_rows, patches):
    part = far * rows_own + patches

    def total(start, rows):
        value = arrived[start : start + rows, :]
        for x in range(1, near):
            value += arrived[x * part + start : x * part + start + rows, :]
        return value

    counts = total(far * rows_own, patches)
    for y in range(far):
        row = y * own_rows
        payload[row : row + rows_own, :] = total(y * rows_own, rows_own)
        payload[row + rows_own : row + rows_own + patches, :] = counts
        rest = own_rows - rows_own - patches
        payload[row + own_rows - rest : row + own_rows, :] = jnp.zeros((rest, PB), jnp.float32)


def route_kernel(
    table, arrived, outgoing, intra, loads, own, left, right, rates,
    *, patches, pair_count, far, group, inverse,
):
    total = arrived[0]
    for y in range(1, far):
        total += arrived[y]
    own[...] = total
    vector_row = 2 * (patches + pair_count)
    counts_row = vector_row + 2
    first = 2 * table[6, 0]
    lines = 2 * patches
    lane = iota((lines, PB), 1)
    line = iota((lines, PB), 0)
    counts = own[counts_row : counts_row + patches, :]
    both = jnp.concatenate([counts, counts], axis=0)
    mine = jnp.sum(jnp.where(lane == first + line // patches, both, 0.0), axis=1, keepdims=True)
    rates[:lines, :] = jnp.broadcast_to(mine, (lines, PB))
    for k in range(pair_count):
        low, high = table[4, k], table[5, k]
        cols = own[pl.ds(counts_row + high, 1), :]
        for r in range(2):
            left[2 * k + r : 2 * k + r + 1, :] = rates[pl.ds(r * patches + low, 1), :]
            right[2 * k + r : 2 * k + r + 1, :] = cols
    rates[...] = fit(own[lines : lines + 2 * pair_count, :], left[...], right[...], inverse)
    terms = []
    for n in range(7):
        row = vector_row + n * group // PB
        at = n * group % PB
        terms.append(own[row : row + 1, at : at + group] * inverse)
    ij, il, jl, ijl, i, j, l = terms
    kappa = ijl - ij * l - il * j - jl * i + 2.0 * i * j * l
    kappa = jnp.concatenate([1000.0 * kappa, jnp.zeros((1, PB - group), jnp.float32)], axis=1)
    base = jnp.where(iota((SLOT_ROWS, PB), 0) == 4, kappa, 0.0)
    for o in range(outgoing.shape[0] // SLOT_ROWS):
        outgoing[o * SLOT_ROWS : (o + 1) * SLOT_ROWS, :] = base
    for k in range(pair_count):
        turned = jnp.full((1, PB), table[7, k].astype(jnp.float32), jnp.float32)
        for m in range(2):
            at = table[m, k]
            outgoing[pl.ds(table[2 + m, k], 1), :] = turned
            for r in range(2):
                outgoing[pl.ds(at + r, 1), :] = rates[2 * k + r : 2 * k + r + 1, :]
    cols = jnp.concatenate([counts[n // 2 : n // 2 + 1, :] for n in range(lines)], axis=0)
    mine = jnp.sum(jnp.where(lane == first + line % 2, cols, 0.0), axis=1, keepdims=True)
    rate = fit(own[:lines, :], mine, cols, inverse)
    intra[...] = rate
    here = lane == (line % 2) * (PB // 2) + table[6, 1] * patches + line // 2
    sums = jnp.sum(rate, axis=1, keepdims=True)
    loads[...] = jnp.sum(jnp.where(here, sums, 0.0), axis=0, keepdims=True)


def owner_kernel(panels, arrived, boundary, loads, cumulant, *, shot_count, far, group):
    for slot in range(2):
        span = pl.ds(slot * PB, PB)
        for r in range(2):
            boundary[pl.ds(slot * PB + r, shot_count, stride=2), :] = arrived[
                pl.ds(2 * slot + r, shot_count, stride=SLOT_ROWS), :
            ]
        straight = boundary[span, :]
        turned = arrived[5 + slot : 6 + slot, :] > 0.5
        boundary[span, :] = jnp.where(turned, straight.T, straight)
    load = jnp.sum(panels[...], axis=0, keepdims=True)
    half = PB // 2
    loads[...] = jnp.concatenate([load[:, :half], load[:, half:]], axis=0)
    for y in range(far):
        row = 2 * y * SLOT_ROWS + 4
        cumulant[:, y * group : (y + 1) * group] = arrived[row : row + 1, :group]


def smem():
    return pl.BlockSpec(memory_space=pltpu.SMEM)


def vmem():
    return pl.BlockSpec(memory_space=pltpu.VMEM)


def f32(*shape):
    return jax.ShapeDtypeStruct(shape, jnp.float32)


def near_f32(*shape):
    return pltpu.VMEM(shape, jnp.float32)


def within(x):
    return pltpu.with_memory_space_constraint(x, pltpu.VMEM)


def exchange(x, axis):
    return lax.all_to_all(x, axis, split_axis=0, concat_axis=0, tiled=True)


def local(events, pair_patches, pair_owners, triples, *, interpret=False):
    shot_dev, det_dev = events.shape
    shot_count = lax.axis_size(SHOT)
    det_count = lax.axis_size("det")
    shot = lax.axis_index(SHOT).astype(jnp.int32).reshape(1)
    panel = lax.axis_index("det").astype(jnp.int32).reshape(1)
    inverse = 1.0 / float(shot_dev * shot_count)
    patches = det_dev // PB
    near = lax.axis_size(SHOT[0])
    far = lax.axis_size(SHOT[1])
    pairs = pair_patches[0].T
    pair_count = pairs.shape[1]
    owners = pair_owners[0].T
    triple_rows = triples.transpose(2, 0, 1)
    triple_count = triple_rows.shape[2]
    group = triple_count // far
    rows_own = 2 * (patches + pair_count) + 2
    own_rows = -(-(rows_own + patches) // 8) * 8
    part = far * rows_own + patches
    chunks = 4

    keep, send, table = pl.pallas_call(
        functools.partial(
            count_kernel,
            chunks=chunks,
            patches=patches,
            pair_count=pair_count,
            near=near,
            far=far,
            rows_own=rows_own,
        ),
        out_shape=(
            near_f32(near * part, PB),
            near_f32(near * part, PB),
            jax.ShapeDtypeStruct((8, pair_count), jnp.int32),
        ),
        in_specs=[pl.BlockSpec(memory_space=pl.ANY)] * 6,
        out_specs=(vmem(), vmem(), pl.BlockSpec(memory_space=pl.ANY)),
        scratch_shapes=[
            pltpu.VMEM((shot_dev, det_dev), jnp.int32),
            pltpu.VMEM((shot_dev, det_dev), jnp.bfloat16),
            pltpu.VMEM((det_dev, shot_dev), jnp.bfloat16),
            pltpu.VMEM((patches * det_dev, PB), jnp.float32),
            pltpu.VMEM((det_dev, 3 * triple_count), jnp.float8_e4m3fn),
            pltpu.SMEM((1,), jnp.int32),
            pltpu.SMEM((1,), jnp.int32),
            pltpu.SMEM((2, pair_count), jnp.int32),
            pltpu.SMEM((2, pair_count), jnp.int32),
            pltpu.SMEM((8, pair_count), jnp.int32),
            pltpu.SMEM((shot_count,), jnp.int32),
            pltpu.VMEM((3, 1, triple_count), jnp.int32),
            pltpu.SemaphoreType.DMA((6,)),
            pltpu.SemaphoreType.DMA((chunks,)),
        ],
        interpret=interpret,
        name="count",
    )(shot, panel, pairs, owners, triple_rows, events)
    other = lax.ppermute(send, SHOT[2], [(0, 1), (1, 0)])
    half = keep + other
    arrived = exchange(half.reshape(near, part, PB), SHOT[0])
    payload = pl.pallas_call(
        functools.partial(
            fold_kernel, near=near, far=far, rows_own=rows_own, own_rows=own_rows, patches=patches
        ),
        out_shape=near_f32(far * own_rows, PB),
        in_specs=[vmem()],
        out_specs=vmem(),
        interpret=interpret,
        name="fold",
    )(within(arrived.reshape(near * part, PB)))
    arrived = exchange(payload.reshape(far, own_rows, PB), SHOT[1])
    outgoing, rates, loads = pl.pallas_call(
        functools.partial(route_kernel, patches=patches, pair_count=pair_count, far=far, group=group, inverse=inverse),
        out_shape=(near_f32(shot_count * SLOT_ROWS, PB), f32(2 * patches, PB), near_f32(1, PB)),
        in_specs=[smem(), vmem()],
        out_specs=(vmem(), vmem(), vmem()),
        scratch_shapes=[
            pltpu.VMEM((own_rows, PB), jnp.float32),
            pltpu.VMEM((2 * pair_count, PB), jnp.float32),
            pltpu.VMEM((2 * pair_count, PB), jnp.float32),
            pltpu.VMEM((2 * pair_count, PB), jnp.float32),
        ],
        interpret=interpret,
        name="route",
    )(table, within(arrived))
    incoming = exchange(outgoing.reshape(shot_count, SLOT_ROWS, PB), SHOT)
    panels = lax.all_gather(loads, "det").reshape(det_count, PB)
    boundary, load, cumulant = pl.pallas_call(
        functools.partial(owner_kernel, shot_count=shot_count, far=far, group=group),
        out_shape=(f32(2 * PB, PB), f32(2, det_count * patches), f32(1, triple_count)),
        in_specs=[vmem(), vmem()],
        out_specs=(vmem(), vmem(), vmem()),
        interpret=interpret,
        name="owner",
    )(within(panels), within(incoming.reshape(SLOT_ROWS * shot_count, PB)))
    return (
        rates.reshape(patches, 2, PB),
        boundary.reshape(1, 1, 2, PB, PB),
        load.T,
        cumulant,
    )


def solution(mesh):
    torus = Mesh(
        mesh.devices.reshape(4, 8, 2, mesh.shape["det"]), ("shot_0", "shot_1", "shot_2", "det")
    )
    return jax.shard_map(
        local,
        mesh=torus,
        in_specs=(P(SHOT, "det"), P("det", None, None), P("det", None, None), P("det", None, None)),
        out_specs=(
            P("det", SHOT, None),
            P("det", SHOT, None, None, None),
            P(None, SHOT),
            P("det", None),
        ),
        check_vma=False,
    )
```
